32 devices in a mesh: batch: 8 (over z, y), vocab: 4 (over x, core).
Axes of the slice: x: 2, y: 2, z: 4, core: 2. Of those that a mesh axis runs over, the one named last changes fastest.
Arguments:
- hidden: bfloat16 [4096, 3584], P(('batch', 'vocab')), may hold values from -6 to 6
- head_weight: bfloat16 [3072, 3584], P('vocab', 'batch'), may hold values from -0.3125 to 0.3125
- targets: int32 [4096], P(('batch', 'vocab')), may hold values from 0 to 3071
- valid_mask: int32 [4096], P(('batch', 'vocab')), may hold values 0 or 1
Outputs:
- head_grad: float32 [3072, 3584], P('vocab', 'batch')
- hidden_grad: float32 [4096, 3584], P(('batch', 'vocab'))
- mean_loss: float32 [], replicated
The draws below stay inside these ranges and needn't reach their ends.
All inputs are finite; a program needn't handle non-finite values. No bound on the sum of `valid_mask` on one device may be relied on, other than what follows from the above.
Results may differ from the reference program's by a relative error of at most 0.0019.
Values may be sent and summed in bfloat16 or wider, within the bound.
No kernel may reach another device: no remote copies, remote signals or barrier semaphores. Data moves between devices by JAX's collectives and lax.ppermute only.
A program may use at most 128 MiB of HBM per device.

```python
import jax
import jax.numpy as jnp
from jax import lax

D = 3584
GROUP_TOK = 512
TOKENS = 4096
VOCAB = 3072
N_BATCH = 8


def set_ends(drawn, stream_key, smallest, top_value):
    spot = [jax.random.randint(jax.random.fold_in(stream_key, axis), (), 0, length) for axis, length in enumerate(drawn.shape)]
    longest = drawn.shape.index(max(drawn.shape))
    neighbour = spot[:longest] + [(spot[longest] + 1) % drawn.shape[longest]] + spot[longest + 1:]
    return drawn.at[tuple(spot)].set(smallest).at[tuple(neighbour)].set(top_value)


def steps_of(rng, dims, split, low, high):
    def one(axis_at, parts):
        steps = jax.random.uniform(jax.random.fold_in(jax.random.fold_in(rng, 6), axis_at), (parts,), jnp.float32, low / len(split), high / len(split))
        return jnp.repeat(jnp.exp(steps), dims[axis_at] // parts).reshape((-1,) + (1,) * (len(dims) - axis_at - 1))

    gain = one(*split[0])
    for cut in split[1:]:
        gain = gain * one(*cut)
    return gain


def normal_values(stream_key, dims, scale, most, shards=(), held_as=jnp.bfloat16):
    factor_of = steps_of(stream_key, dims, shards, -0.22, 0.18) if shards else 1.0
    array = jax.random.normal(stream_key, dims, jnp.float32) * scale * factor_of
    return jnp.minimum(jnp.maximum(array, -most), most).astype(held_as)


def setup_inputs(seed: int = 0) -> dict:
    arg_keys = jax.random.split(jax.random.key(seed), 5)
    hidden = normal_values(arg_keys[0], (TOKENS, D), 1.0, 6.0, ((0, 32),))
    head_weight = normal_values(arg_keys[1], (VOCAB, D), (D // 9) ** -0.5, 0.3125, ((0, 4), (1, 8)))
    targets = set_ends(jax.random.randint(arg_keys[2], (TOKENS,), 0, VOCAB), jax.random.fold_in(arg_keys[2], 1), 0, VOCAB - 1).astype(jnp.int32)
    valid_mask = set_ends((jax.random.randint(arg_keys[3], (TOKENS,), 0, 4) < 3).astype(jnp.int32), jax.random.fold_in(arg_keys[3], 1), 0, 1)
    return {"hidden": hidden, "head_weight": head_weight, "targets": targets, "valid_mask": valid_mask}


softcap = 30.0


def reference(hidden, head_weight, targets, valid_mask):
    positions = hidden.shape[0]
    model_width = hidden.shape[1]
    state_blocks = hidden.reshape(N_BATCH, GROUP_TOK, model_width)
    target_blocks = targets.reshape(N_BATCH, GROUP_TOK)
    mask_blocks = valid_mask.reshape(N_BATCH, GROUP_TOK)
    vocab_ids = jnp.arange(VOCAB, dtype=jnp.int32)

    def token_block(running, scanned):
        grad_total, loss_total = running
        row_block, target_ids, mask_block = scanned
        scores = lax.dot_general(row_block, head_weight, (((1,), (1,)), ((), ())), preferred_element_type=jnp.float32)
        logits = softcap * jnp.tanh(scores / softcap)
        target_hit = vocab_ids[None, :] == target_ids[:, None]
        exponent = jnp.exp(logits)
        partition = jnp.sum(exponent, axis=1)
        target_logit = jnp.sum(jnp.where(target_hit, logits, 0.0), axis=1)
        weight = mask_block.astype(jnp.float32)
        slope = 1.0 - (logits / softcap) ** 2
        delta_logit = (weight[:, None] * (exponent / partition[:, None] - target_hit.astype(jnp.float32)) * slope).astype(jnp.bfloat16)
        grad_total = grad_total + lax.dot_general(delta_logit, row_block, (((0,), (0,)), ((), ())), preferred_element_type=jnp.float32)
        loss_total = loss_total + jnp.sum(weight * (jnp.log(partition) - target_logit))
        state_grad = jnp.dot(delta_logit, head_weight, preferred_element_type=jnp.float32)
        return (grad_total, loss_total), state_grad

    start_grad = jnp.zeros(head_weight.shape, jnp.float32)
    start_loss = jnp.zeros((), jnp.float32)
    (head_grad, loss_total), state_grads = lax.scan(token_block, (start_grad, start_loss), (state_blocks, target_blocks, mask_blocks))
    hidden_grad = state_grads.reshape(positions, model_width)
    mean_loss = loss_total / positions
    return head_grad, hidden_grad, mean_loss
```

```python
import math

import jax
import jax.numpy as jnp
from jax import lax
from jax.sharding import Mesh, PartitionSpec as P

softcap = 30.0


def capped(scores):
    return softcap * jnp.tanh(scores / softcap)


def xor_send(value, axis, bit):
    size = lax.axis_size(axis)
    return lax.ppermute(value, axis, [(i, i ^ bit) for i in range(size)])


def bits_of(axis):
    size = lax.axis_size(axis)
    assert size & (size - 1) == 0
    return [1 << k for k in range(size.bit_length() - 1)]


def arrival_tables(length):
    tables = []
    for at in range(length):
        order = []
        for step in range(1, length):
            if at - step >= 0:
                order.append(("up", step))
            if at + step < length:
                order.append(("down", step))
        tables.append(order)
    return tables


def line_gather(block, rider=None, hops=(), shares=None):
    length = lax.axis_size("z")
    width = lax.axis_size("y")
    z = lax.axis_index("z")
    y = lax.axis_index("y")
    ups = [(i, i + 1) for i in range(length - 1)]
    downs = [(i + 1, i) for i in range(length - 1)]
    seen = {}
    hops = list(hops)
    hops_each = -(-len(hops) // max(length - 2, 1))
    first = min(2, length - 1)
    up = down = block
    for step in range(1, length):
        up = lax.ppermute(up, "z", ups[step - 1:])
        down = lax.ppermute(down, "z", downs[: length - step])
        if rider is not None:
            for axis, bit in hops[max(step - first, 0) * hops_each: max(step - first + 1, 0) * hops_each]:
                rider = rider + xor_send(rider, axis, bit)
            if step == min(3, length - 1):
                for bit in bits_of("x"):
                    kept, sent = shares if bit == 1 else jnp.split(shares, 2, axis=0)
                    shares = kept + xor_send(sent, "x", bit)
            up, down, rider, shares = lax.optimization_barrier((up, down, rider, shares))
        seen["up", step] = up
        seen["down", step] = down
    tables = arrival_tables(length)
    found = [(z, block)]
    for nth in range(length - 1):
        choice = None
        source = None
        for key in dict.fromkeys(table[nth] for table in tables):
            here = jnp.zeros((), bool)
            for at in range(length):
                if tables[at][nth] == key:
                    here = here | (z == at)
            origin = z - key[1] if key[0] == "up" else z + key[1]
            if choice is None:
                choice, source = seen[key], origin
            else:
                choice = jnp.where(here, seen[key], choice)
                source = jnp.where(here, origin, source)
        found.append((source, choice))
    out = []
    for source, value in found:
        out.append((source, y, value))
        for shift in range(1, width):
            moved = lax.ppermute(value, "y", [(i, (i + shift) % width) for i in range(width)])
            out.append((source, (y - shift) % width, moved))
    return out, rider, shares


def vocab_gather(block):
    parts = [block]
    for bit in reversed(bits_of("x")):
        parts = parts + [xor_send(part, "x", bit) for part in parts]
    return parts + [xor_send(part, "c", 1) for part in parts]


def local(hidden, head_weight, targets, valid_mask):
    own_tokens, width = hidden.shape
    own_rows, own_cols = head_weight.shape
    wide = lax.axis_size("y")
    batch_count = lax.axis_size("z") * wide
    group_size = lax.axis_size("x") * lax.axis_size("c")
    batch_index = lax.axis_index("z") * wide + lax.axis_index("y")
    vocab_index = lax.axis_index("x") * lax.axis_size("c") + lax.axis_index("c")
    group_tokens = own_tokens * group_size

    packed = jnp.concatenate(vocab_gather(targets * 2 + valid_mask))
    states = jnp.concatenate(vocab_gather(hidden), axis=0)
    group_ids = packed >> 1
    weight = (packed & 1).astype(jnp.float32)

    head = jnp.zeros((own_rows, width), head_weight.dtype)
    for z, y, value in line_gather(head_weight)[0]:
        head = lax.dynamic_update_slice(head, value, (0, (z * wide + y) * own_cols))

    pieces = jnp.transpose(hidden.reshape(own_tokens, batch_count, own_cols), (1, 0, 2))
    own_columns = jnp.zeros_like(pieces)
    for offset in range(batch_count):
        other = batch_index ^ offset
        piece = lax.dynamic_index_in_dim(pieces, other, 0, keepdims=True)
        if offset:
            piece = lax.ppermute(piece, ("z", "y"), [(i, i ^ offset) for i in range(batch_count)])
        own_columns = lax.dynamic_update_slice(own_columns, piece, (other, 0, 0))
    own_columns, head = lax.optimization_barrier((own_columns, head))

    scores = lax.dot_general(
        states, head, (((1,), (1,)), ((), ())), preferred_element_type=jnp.float32
    )
    logits = capped(scores)
    columns = jnp.arange(own_rows, dtype=jnp.int32)
    target_hit = columns[None, :] == (group_ids - vocab_index * own_rows)[:, None]
    exponent = jnp.exp(logits)
    sums = jnp.stack(
        [jnp.sum(exponent, axis=1), jnp.sum(jnp.where(target_hit, logits, 0.0), axis=1)]
    ).reshape(2, 2, group_size // 2, own_tokens)
    sums = sums + jnp.flip(xor_send(sums, "c", 1), axis=1)
    for bit in bits_of("x"):
        sums = sums + half_swap(xor_send(sums, "x", bit), bit)
    partition, target_logit = sums.reshape(2, group_tokens)
    slope = 1.0 - (logits / softcap) ** 2
    delta_logit = (
        weight[:, None] * (exponent / partition[:, None] - target_hit.astype(jnp.float32)) * slope
    ).astype(jnp.bfloat16)

    column_parts = [own_columns]
    for bit in reversed(bits_of("x")):
        column_parts = column_parts + [xor_send(part, "x", bit) for part in column_parts]
    delta_logit, column_parts = lax.optimization_barrier((delta_logit, column_parts))
    sent_columns = [xor_send(part, "c", 1) for part in column_parts]

    all_delta = jnp.zeros((batch_count, group_tokens, own_rows), jnp.bfloat16)
    own_loss = weight[:own_tokens] * (jnp.log(partition[:own_tokens]) - target_logit[:own_tokens])
    loss = jnp.sum(own_loss).reshape(1, 1)
    hops = [(axis, bit) for axis in ("c", "x", "y", "z") for bit in bits_of(axis)]
    partial_grad = jnp.dot(delta_logit, head, preferred_element_type=jnp.float32)
    kept, sent = jnp.split(partial_grad, 2, axis=0)
    kept = jnp.split(kept + xor_send(sent, "c", 1), 2, axis=0)
    blocks, loss, hidden_grad = line_gather(delta_logit, loss, hops, kept)
    for z, y, value in blocks:
        all_delta = lax.dynamic_update_slice(all_delta, value[None], (z * wide + y, 0, 0))

    group_columns = jnp.concatenate(column_parts + sent_columns, axis=1)

    head_grad = lax.dot_general(
        all_delta.reshape(-1, own_rows),
        group_columns.reshape(-1, own_cols),
        (((0,), (0,)), ((), ())),
        preferred_element_type=jnp.float32,
    )

    mean_loss = loss[0, 0] / (group_tokens * batch_count)
    return (head_grad, hidden_grad, mean_loss)


def half_swap(sums, bit):
    kinds, halves, count, tokens = sums.shape
    positions = [0]
    for step in reversed(bits_of("x")):
        positions = positions + [position ^ step for position in positions]
    index = [positions.index(position ^ bit) for position in positions]
    return jnp.concatenate([sums[:, :, i:i + 1] for i in index], axis=2)


def solution(mesh):
    batch, vocab = mesh.shape["batch"], mesh.shape["vocab"]
    cores = 2
    wide = 1 << (int(math.log2(batch)) // 2)
    split = Mesh(
        mesh.devices.reshape(batch // wide, wide, vocab // cores, cores), ("z", "y", "x", "c")
    )
    batch_axes, vocab_axes = ("z", "y"), ("x", "c")
    everything = batch_axes + vocab_axes
    placed = (P(everything, None), P(vocab_axes, batch_axes), P(everything), P(everything))
    return jax.shard_map(
        local,
        mesh=split,
        in_specs=placed,
        out_specs=(P(vocab_axes, batch_axes), P(everything, None), P()),
        check_vma=False,
    )
```
